512 devices in a mesh: mode: 32 (over z_hi, y), space: 16 (over x, z_lo, core).
Axes of the slice: x: 4, y: 8, z: 8 (z_hi: 4, z_lo: 2; z = z_hi * 2 + z_lo), core: 2. Of those that a mesh axis runs over, the one named last changes fastest.
Arguments:
- pressure: float32 [512, 32, 4, 128], P('mode', 'space'), may hold values from -6 to 6
- source: float32 [512, 32, 4, 128], P('mode', 'space'), may hold values from -6 to 6
- coefficients: float32 [32, 32, 4, 128], P(None, 'space'), may hold values from 0.2 to 2
- coupling: float32 [32, 512, 512], P(None, 'mode'), as said below
Outputs:
- pressure_out: float32 [512, 32, 4, 128], P('mode', 'space')
- residual: float32 [512, 32, 4, 128], P('mode', 'space')
The draws below stay inside these ranges and needn't reach their ends.
Inputs may be any that keep to these rules, and one draw needn't show every extreme that they name: coupling[k] is symmetric for every k.
All inputs are finite; a program needn't handle non-finite values.
Results may differ from the reference program's by a relative error of at most 0.00011.
Values sent between devices are 32-bit elements; how exact they have to be, the bound alone decides.
A program may use at most 64 MiB of HBM per device.

```python
import math
import jax
import jax.numpy as jnp
from jax import lax

P_SIZE = 512
TERMS = 32
ITERS = 2
CY = 4
CZ = 128
NX = 32


def draw_coupling(key, part):
    raw = jax.random.normal(key, (TERMS, P_SIZE, P_SIZE), jnp.float32)
    symmetric = (raw + jnp.swapaxes(raw, 1, 2)) * (0.5 / jnp.sqrt(2.0 * P_SIZE))
    rows = lax.broadcasted_iota(jnp.int32, (TERMS, P_SIZE, P_SIZE), 1)
    cols = lax.broadcasted_iota(jnp.int32, (TERMS, P_SIZE, P_SIZE), 2)
    terms = lax.broadcasted_iota(jnp.int32, (TERMS, P_SIZE, P_SIZE), 0)
    identity = jnp.where((rows == cols) & (terms == 0), 1.0, 0.0).astype(jnp.float32)
    return symmetric + identity


def block_levels(key, shape, shards, low, largest):
    level = 1.0
    for position, shards_of in shards:
        heights = jax.random.uniform(jax.random.fold_in(jax.random.fold_in(key, 6), position), (shards_of,), jnp.float32, low / len(shards), largest / len(shards))
        level = level * jnp.repeat(jnp.exp(heights), shape[position] // shards_of).reshape((-1,) + (1,) * (len(shape) - 1 - position))
    return level


def normal_values(stream_key, shape, scale, most, split=(), dtype=jnp.bfloat16):
    drawn = jax.random.normal(stream_key, shape, jnp.float32) * scale
    if len(split) > 0:
        drawn = block_levels(stream_key, shape, split, -0.22, 0.18) * drawn
    return jnp.clip(drawn, min=-most, max=most).astype(dtype)


def setup_inputs(seed: int = 0) -> dict:
    arg_keys = jax.random.split(jax.random.key(seed), 5)
    pressure = normal_values(arg_keys[0], (P_SIZE, NX, CY, CZ), 1.0, 6.0, ((0, 32), (1, 16)), jnp.float32)
    source = normal_values(arg_keys[1], (P_SIZE, NX, CY, CZ), 1.0, 6.0, ((0, 32), (1, 16)), jnp.float32)
    coefficients = jnp.clip(jnp.exp(math.log(2.0) - 2.3025851 * jax.random.uniform(arg_keys[2], (TERMS, NX, CY, CZ), jnp.float32) ** block_levels(arg_keys[2], (TERMS, NX, CY, CZ), ((1, 16),), -0.2, 0.2)), 0.2, 2.0)
    coupling = draw_coupling(jax.random.fold_in(arg_keys[4], 71), 0)
    return {"pressure": pressure, "source": source, "coefficients": coefficients, "coupling": coupling}


storage_coef = 1.0
damping = 0.7


def shifted(padded, spatial_axis, offset):
    index = [slice(None)] * padded.ndim
    for place in (-3, -2, -1):
        index[place] = slice(1, padded.shape[place] - 1)
    index[spatial_axis] = slice(1 + offset, padded.shape[spatial_axis] - 1 + offset)
    return padded[tuple(index)]


def yz_pad(array):
    return jnp.pad(array, [(0, 0)] * (array.ndim - 2) + [(1, 1), (1, 1)])


def local_stencil(coef_x, field_x):
    coef_p = yz_pad(coef_x)
    field_p = yz_pad(field_x)
    centre_c = shifted(coef_p, -3, 0)
    centre_f = shifted(field_p, -3, 0)
    total = None
    for spatial_axis in (-3, -2, -1):
        for offset in (-1, 1):
            term = 0.5 * (centre_c + shifted(coef_p, spatial_axis, offset)) * (centre_f - shifted(field_p, spatial_axis, offset))
            total = term if total is None else total + term
    return total


def face_total(coef_x):
    coef_p = yz_pad(coef_x)
    centre_c = shifted(coef_p, -3, 0)
    total = jnp.zeros(centre_c.shape, jnp.float32)
    for spatial_axis in (-3, -2, -1):
        for offset in (-1, 1):
            total = total + 0.5 * (centre_c + shifted(coef_p, spatial_axis, offset))
    return total


def x_pad(array):
    return jnp.pad(array, [(0, 0), (1, 1), (0, 0), (0, 0)])


def reference(pressure, source, coefficients, coupling):
    coef_x = x_pad(coefficients)
    mean_x = coef_x[0]
    diag = storage_coef + face_total(mean_x)
    residual = source
    for outer in range(ITERS):
        press_x = x_pad(pressure)

        def add_term(total, inputs):
            coef_k, matrix = inputs
            mixed = jnp.einsum('ij,jxyz->ixyz', matrix, press_x, precision=lax.Precision.HIGHEST)
            return total + local_stencil(coef_k[None], mixed), None

        applied = lax.scan(add_term, jnp.zeros(pressure.shape, jnp.float32), (coef_x, coupling))[0]
        residual = source - storage_coef * pressure - applied
        first = damping * residual / diag
        mean_apply = storage_coef * first + local_stencil(mean_x[None], x_pad(first))
        second = first + damping * (residual - mean_apply) / diag
        pressure = pressure + second
    return pressure, residual
```

```python
import functools

import jax
import jax.numpy as jnp
from jax import lax
from jax.experimental import pallas as pl
from jax.experimental.pallas import tpu as pltpu
from jax.sharding import PartitionSpec as P

MESH = pl.DeviceIdType.MESH
ITERS = 2
DAMP = 0.7
KT, IB, PM = 32, 16, 512
NY, NZ = 8, 4
CELLS = 1024
SPLIT = 768
F32, BF16 = jnp.float32, jnp.bfloat16

AZ = 0
AR = AZ + 3
AL = AR + 16
BR = AL + 16
BL = BR + 4
BZ = BL + 4
NMSG = BZ + 24


def lanes_next(v):
    n = v.shape[-1]
    lane = lax.broadcasted_iota(jnp.int32, v.shape, v.ndim - 1)
    return jnp.where(lane < n - 1, pltpu.roll(v, n - 1, v.ndim - 1), 0.0)


def lanes_prev(v):
    lane = lax.broadcasted_iota(jnp.int32, v.shape, v.ndim - 1)
    return jnp.where(lane > 0, pltpu.roll(v, 1, v.ndim - 1), 0.0)


def split_bf16(x):
    hi = x.astype(BF16)
    return hi, (x - hi.astype(F32)).astype(BF16)


def kernel(u_ref, src_ref, a_ref, c_ref, po_ref, ro_ref,
           ug, a_halo, c_hi, c_lo, faces, dinv, m_ref, uh_ref, ul_ref,
           hs_send, hs_recv, out_u, src_m,
           gs, gr, hss, hsr, cs, cr):
    mode, space = lax.axis_index("mode"), lax.axis_index("space")
    ns = lax.axis_size("space")
    zh, y = mode // NY, lax.rem(mode, NY)
    left_s, right_s = lax.rem(space + ns - 1, ns), lax.rem(space + 1, ns)
    yr = zh * NY + lax.rem(y + 1, NY)
    yl = zh * NY + lax.rem(y + NY - 1, NY)

    def at_z(q):
        return lax.rem(zh + q, NZ) * NY + y

    def block(q, d):
        return lax.rem(zh + q, NZ) * NY + lax.rem(y + NY + d, NY)

    barrier = pltpu.get_barrier_semaphore()
    for target in (yr, yl, at_z(1), at_z(2), at_z(3)):
        pl.semaphore_signal(barrier, inc=1, device_id={"mode": target, "space": space}, device_id_type=MESH)
    for target in (left_s, right_s):
        pl.semaphore_signal(barrier, inc=1, device_id={"mode": mode, "space": target}, device_id_type=MESH)

    for s in range(8):
        ug[0, mode, :, s * 128:(s + 1) * 128] = u_ref[:, s, :]
        src_m[:, s * 128:(s + 1) * 128] = src_ref[:, s, :]
    pl.semaphore_wait(barrier, 7)

    def coef_copy(side):
        target = right_s if side == 0 else left_s
        return pltpu.make_async_remote_copy(
            src_ref=a_ref, dst_ref=a_halo.at[side], send_sem=cs.at[side], recv_sem=cr.at[side],
            device_id={"mode": mode, "space": target}, device_id_type=MESH)

    def halo_copy(it, side):
        target = right_s if side == 0 else left_s
        return pltpu.make_async_remote_copy(
            src_ref=hs_send.at[it, side], dst_ref=hs_recv.at[it, side],
            send_sem=hss.at[it, side], recv_sem=hsr.at[it, side],
            device_id={"mode": mode, "space": target}, device_id_type=MESH)

    acols, bcols = slice(0, SPLIT), slice(SPLIT, CELLS)

    def gather(it):
        sent = []

        def msg(number, b, cols, target):
            return pltpu.make_async_remote_copy(
                src_ref=ug.at[it, b, :, cols], dst_ref=ug.at[it, b, :, cols],
                send_sem=gs.at[it, number], recv_sem=gr.at[it, number],
                device_id={"mode": target, "space": space}, device_id_type=MESH)

        def send(number, b, cols, target):
            copy = msg(number, b, cols, target)
            copy.start()
            sent.append(copy)

        def arrive(number, b, cols):
            msg(number, b, cols, yr).wait_recv()

        limit_r = [4, 3, 4, 3]
        limit_l = [3, 4, 3, 4]

        def a_right(q, t):
            send(AR + q * 4 + t - 1, block(q, -(t - 1)), acols, yr)

        def a_left(q, t):
            send(AL + q * 4 + t - 1, block(q, t - 1), acols, yl)

        def b_z(d):
            for q in (1, 2, 3):
                send(BZ + (d % NY) * 3 + q - 1, block(0, d), bcols, at_z(q))

        for q in (1, 3, 2):
            send(AZ + q - 1, mode, acols, at_z(q))
        send(BR + 0, mode, bcols, yr)
        send(BL + 0, mode, bcols, yl)
        a_right(0, 1)
        a_left(0, 1)
        b_z(0)
        for q in (1, 3, 2):
            arrive(AZ + q - 1, block(NZ - q, 0), acols)
            a_right(NZ - q, 1)
            a_left(NZ - q, 1)
        for t in (1, 2, 3, 4):
            if t <= 4:
                arrive(BR + t - 1, block(0, -t), bcols)
                if t < 4:
                    send(BR + t, block(0, -t), bcols, yr)
                b_z(-t)
            if t <= 3:
                arrive(BL + t - 1, block(0, t), bcols)
                if t < 3:
                    send(BL + t, block(0, t), bcols, yl)
                b_z(t)
            for q in (0, 3, 1, 2):
                if t <= limit_r[q]:
                    arrive(AR + q * 4 + t - 1, block(q, -t), acols)
                    if t < limit_r[q]:
                        a_right(q, t + 1)
                if t <= limit_l[q]:
                    arrive(AL + q * 4 + t - 1, block(q, t), acols)
                    if t < limit_l[q]:
                        a_left(q, t + 1)
        for d in range(NY):
            for q in (1, 2, 3):
                arrive(BZ + d * 3 + q - 1, block(NZ - q, d), bcols)
        return sent

    def prepare():
        for r in range(8):
            rows = slice(r * 64, (r + 1) * 64)
            hi, lo = split_bf16(c_ref[rows, :])
            c_hi[rows, :] = hi
            c_lo[rows, :] = lo
        coef_copy(0).wait_recv()
        coef_copy(1).wait_recv()
        sub = lax.broadcasted_iota(jnp.int32, (8, 128), 0)
        ysub = lax.rem(sub, 4)
        plane0 = sub < 4
        has_l, has_r = space > 0, space < ns - 1

        def one(k, _):
            a = a_ref[k]
            al = jnp.where(has_l, a_halo[0, k], 0.0)
            ar = jnp.where(has_r, a_halo[1, k], 0.0)
            a4 = pltpu.roll(a, 4, 0)
            xm = jnp.where(plane0, pltpu.roll(al, 4, 0), a4)
            xp = jnp.where(plane0, a4, pltpu.roll(ar, 4, 0))
            ym = jnp.where(ysub > 0, pltpu.roll(a, 1, 0), 0.0)
            yp = jnp.where(ysub < 3, pltpu.roll(a, 7, 0), 0.0)
            for n, v in enumerate((xm, xp, ym, yp, lanes_prev(a), lanes_next(a))):
                faces[n, k] = 0.5 * (a + v)
            return 0

        lax.fori_loop(0, KT, one, 0)

        def face_sum(a, x_nb):
            total = x_nb
            total = total + jnp.where(ysub > 0, pltpu.roll(a, 1, 0), 0.0)
            total = total + jnp.where(ysub < 3, pltpu.roll(a, 7, 0), 0.0)
            total = total + lanes_prev(a) + lanes_next(a)
            return 1.0 + 0.5 * (6.0 * a + total)

        a = a_ref[0]
        al = jnp.where(has_l, a_halo[0, 0], 0.0)
        ar = jnp.where(has_r, a_halo[1, 0], 0.0)
        a4, al4, ar4 = pltpu.roll(a, 4, 0), pltpu.roll(al, 4, 0), pltpu.roll(ar, 4, 0)
        dinv[0] = DAMP / face_sum(a, a4 + jnp.where(plane0, al4, ar4))
        dinv[1] = DAMP / face_sum(al, a4 + al4)
        dinv[2] = DAMP / face_sum(ar, a4 + ar4)

    def mixed(it):
        for r in range(8):
            x = ug[it, r * 4:(r + 1) * 4].reshape(64, CELLS)
            hi, lo = split_bf16(x)
            uh_ref[r * 64:(r + 1) * 64, :] = hi
            ul_ref[r * 64:(r + 1) * 64, :] = lo
        for t in range(4):
            cols = slice(t * 256, (t + 1) * 256)
            uh, ul = uh_ref[:, cols], ul_ref[:, cols]
            acc = jnp.dot(c_hi[...], uh, preferred_element_type=F32)
            acc += jnp.dot(c_hi[...], ul, preferred_element_type=F32)
            acc += jnp.dot(c_lo[...], uh, preferred_element_type=F32)
            m_ref[:, cols] = acc

    def sums(s):
        def one(k, acc):
            m = m_ref[pl.ds(pl.multiple_of(k * IB, IB), IB), s * 128:(s + 1) * 128]
            return tuple(acc[n] + faces[n, k, s:s + 1, :] * m for n in range(6))

        zero = jnp.zeros((IB, 128), F32)
        return lax.fori_loop(0, KT, one, (zero,) * 6, unroll=4)

    def tile(s):
        return slice(s * 128, (s + 1) * 128)

    coef_copy(0).start()
    coef_copy(1).start()
    sent = []
    has_l = space > 0
    has_r = space < ns - 1
    for it in range(ITERS):
        sent += gather(it)
        if it == 0:
            prepare()
        mixed(it)
        S = [sums(s) for s in range(8)]
        own = [ug[it, mode, :, tile(s)] for s in range(8)]
        part = []
        for s in range(8):
            xm, xp, ym, yp, zm, zp = S[s]
            ap = (xm + xp) + (ym + yp) + (zm + zp)
            ap = ap - (S[s + 4][0] if s < 4 else S[s - 4][1])
            if s % 4 < 3:
                ap = ap - S[s + 1][2]
            if s % 4 > 0:
                ap = ap - S[s - 1][3]
            ap = ap - lanes_next(zm) - lanes_prev(zp)
            part.append(src_m[:, tile(s)] - own[s] - ap)
        for c in range(4):
            hs_send[it, 0, :, tile(c)] = S[4 + c][1]
            hs_send[it, 0, :, tile(4 + c)] = part[4 + c]
            hs_send[it, 1, :, tile(c)] = S[c][0]
            hs_send[it, 1, :, tile(4 + c)] = part[c]
        halo_copy(it, 0).start()
        halo_copy(it, 1).start()
        halo_copy(it, 0).wait_recv()
        halo_copy(it, 1).wait_recv()
        res, first = [], []
        left_first, right_first = [], []
        for c in range(4):
            res.append(part[c] + jnp.where(has_l, hs_recv[it, 0, :, tile(c)], 0.0))
            v = (hs_recv[it, 0, :, tile(4 + c)] + S[c][0]) * dinv[1, 4 + c:5 + c, :]
            left_first.append(jnp.where(has_l, v, 0.0))
        for c in range(4):
            res.append(part[4 + c] + jnp.where(has_r, hs_recv[it, 1, :, tile(c)], 0.0))
            v = (hs_recv[it, 1, :, tile(4 + c)] + S[4 + c][1]) * dinv[2, c:c + 1, :]
            right_first.append(jnp.where(has_r, v, 0.0))
        for s in range(8):
            first.append(res[s] * dinv[0, s:s + 1, :])
        for s in range(8):
            f = first[s]
            fc = [faces[n, 0, s:s + 1, :] for n in range(6)]
            ap = f
            ap = ap + fc[0] * (f - (first[s - 4] if s >= 4 else left_first[s]))
            ap = ap + fc[1] * (f - (first[s + 4] if s < 4 else right_first[s - 4]))
            ap = ap + fc[2] * (f - first[s - 1] if s % 4 > 0 else f)
            ap = ap + fc[3] * (f - first[s + 1] if s % 4 < 3 else f)
            ap = ap + fc[4] * (f - lanes_prev(f))
            ap = ap + fc[5] * (f - lanes_next(f))
            second = f + (res[s] - ap) * dinv[0, s:s + 1, :]
            new = own[s] + second
            if it + 1 < ITERS:
                ug[it + 1, mode, :, tile(s)] = new
            else:
                po_ref[:, s, :] = new
                ro_ref[:, s, :] = res[s]
    for copy in sent:
        copy.wait_send()
    for side in (0, 1):
        coef_copy(side).wait_send()
        for it in range(ITERS):
            halo_copy(it, side).wait_send()


def on_device(pressure, source, coefficients, coupling):
    vmem = pl.BlockSpec(memory_space=pltpu.VMEM)
    shape = jax.ShapeDtypeStruct((IB, 8, 128), F32)
    dma = pltpu.SemaphoreType.DMA
    out = pl.pallas_call(
        kernel,
        out_shape=(shape, shape),
        in_specs=[vmem] * 4,
        out_specs=(vmem, vmem),
        scratch_shapes=[
            pltpu.VMEM((ITERS, PM // IB, IB, CELLS), F32),
            pltpu.VMEM((2, KT, 8, 128), F32),
            pltpu.VMEM((PM, PM), BF16),
            pltpu.VMEM((PM, PM), BF16),
            pltpu.VMEM((6, KT, 8, 128), F32),
            pltpu.VMEM((3, 8, 128), F32),
            pltpu.VMEM((PM, CELLS), F32),
            pltpu.VMEM((PM, CELLS), BF16),
            pltpu.VMEM((PM, CELLS), BF16),
            pltpu.VMEM((ITERS, 2, IB, CELLS), F32),
            pltpu.VMEM((ITERS, 2, IB, CELLS), F32),
            pltpu.VMEM((IB, CELLS), F32),
            pltpu.VMEM((IB, CELLS), F32),
            dma((ITERS, NMSG)),
            dma((ITERS, NMSG)),
            dma((ITERS, 2)),
            dma((ITERS, 2)),
            dma((2,)),
            dma((2,)),
        ],
        compiler_params=pltpu.CompilerParams(
            collective_id=0, has_side_effects=True, vmem_limit_bytes=40 * 1024 * 1024),
    )(pressure.reshape(IB, 8, 128), source.reshape(IB, 8, 128),
      coefficients.reshape(KT, 8, 128), coupling.reshape(PM, PM))
    return tuple(o.reshape(IB, 2, 4, 128) for o in out)


def solution(mesh):
    return jax.shard_map(
        on_device, mesh=mesh,
        in_specs=(P("mode", "space", None, None), P("mode", "space", None, None),
                  P(None, "space", None, None), P(None, "mode", None)),
        out_specs=(P("mode", "space", None, None), P("mode", "space", None, None)),
        check_vma=False)
```

```python
import functools

import jax
import jax.numpy as jnp
from jax import lax
from jax.experimental import pallas as pl
from jax.experimental.pallas import tpu as pltpu
from jax.sharding import PartitionSpec as P

MESH = pl.DeviceIdType.MESH
ITERS = 2
DAMP = 0.7
KT, IB, PM = 32, 16, 512
NY, NZ = 8, 4
CELLS = 1024
F32, BF16 = jnp.float32, jnp.bfloat16

APIECES = [slice(0, 384), slice(384, 768)]
BPIECE = slice(768, 1024)
ZORDER = (2, 1, 3)
OFF = [0, 0.8, 1.2, 0.8]
NA = 35
NB0 = NA * len(APIECES)
NMSG = NB0 + 32

SLOT = list(range(NY))


def lanes_next(v):
    n = v.shape[-1]
    lane = lax.broadcasted_iota(jnp.int32, v.shape, v.ndim - 1)
    return jnp.where(lane < n - 1, pltpu.roll(v, n - 1, v.ndim - 1), 0.0)


def lanes_prev(v):
    lane = lax.broadcasted_iota(jnp.int32, v.shape, v.ndim - 1)
    return jnp.where(lane > 0, pltpu.roll(v, 1, v.ndim - 1), 0.0)


def split_bf16(x):
    hi = x.astype(BF16)
    return hi, (x - hi.astype(F32)).astype(BF16)


def kernel(u_hbm, src_hbm, a_hbm, c_hbm, po_ref, ro_ref,
           u_ref, src_ref, a_ref, c_ref,
           ug, a_halo, c_st, faces, dinv, m_ref, u_st,
           hs_send, hs_recv, src_m,
           ls, gs, gr, hss, hsr, cs, cr):
    mode, space = lax.axis_index("mode"), lax.axis_index("space")
    ns = lax.axis_size("space")
    zh, y = mode // NY, lax.rem(mode, NY)
    left_s, right_s = lax.rem(space + ns - 1, ns), lax.rem(space + 1, ns)
    yr = zh * NY + lax.rem(y + 1, NY)
    yl = zh * NY + lax.rem(y + NY - 1, NY)
    has_l, has_r = space > 0, space < ns - 1

    def at_z(q):
        return lax.rem(zh + q, NZ) * NY + y

    def block(q, d):
        return lax.rem(zh + q, NZ) * NY + lax.rem(y + NY + d, NY)

    barrier = pltpu.get_barrier_semaphore()
    for target in (yr, yl, at_z(1), at_z(2), at_z(3)):
        pl.semaphore_signal(barrier, inc=1, device_id={"mode": target, "space": space}, device_id_type=MESH)
    for target in (left_s, right_s):
        pl.semaphore_signal(barrier, inc=1, device_id={"mode": mode, "space": target}, device_id_type=MESH)

    loads = [pltpu.make_async_copy(h, v, ls.at[n]) for n, (h, v) in enumerate(
        ((u_hbm, u_ref), (a_hbm, a_ref), (c_hbm, c_ref), (src_hbm, src_ref)))]
    for copy in loads:
        copy.start()

    def tile(s):
        return slice(s * 128, (s + 1) * 128)

    loads[0].wait()
    for s in range(8):
        ug[0, mode, :, tile(s)] = u_ref[:, s, :]
    loads[1].wait()

    def own_faces(k, _):
        a = a_ref[k]
        a4 = pltpu.roll(a, 4, 0)
        sub8 = lax.rem(lax.broadcasted_iota(jnp.int32, (8, 128), 0), 4)
        ym = jnp.where(sub8 > 0, pltpu.roll(a, 1, 0), 0.0)
        yp = jnp.where(sub8 < 3, pltpu.roll(a, 7, 0), 0.0)
        for n, v in enumerate((a4, a4, ym, yp, lanes_prev(a), lanes_next(a))):
            faces[n, k] = 0.5 * (a + v)
        return 0

    lax.fori_loop(0, KT, own_faces, 0, unroll=8)

    loads[2].wait()
    for r in range(8):
        rows = slice(r * 64, (r + 1) * 64)
        hi, lo = [], []
        for q in range(NZ):
            cols = pl.ds(pl.multiple_of(lax.rem(zh + q, NZ) * 128, 128), 128)
            x = pltpu.roll(c_ref[rows, cols], lax.rem(NY - y, NY) * IB, 1)
            h = x.astype(BF16).astype(F32)
            hi.append(h)
            lo.append(x - h)
        for d in range(NY):
            part = slice(d * IB, (d + 1) * IB)
            h = jnp.concatenate([v[:, part] for v in hi], axis=1)
            l = jnp.concatenate([v[:, part] for v in lo], axis=1)
            c_st[SLOT[d], rows, 0:64] = h.astype(BF16)
            c_st[SLOT[d], rows, 64:128] = h.astype(BF16)
            c_st[SLOT[d], rows, 128:192] = l.astype(BF16)
    loads[3].wait()
    for s in range(8):
        src_m[:, tile(s)] = src_ref[:, s, :]
    pl.semaphore_wait(barrier, 7)

    def coef_copy(side):
        target = right_s if side == 0 else left_s
        return pltpu.make_async_remote_copy(
            src_ref=a_ref, dst_ref=a_halo.at[side], send_sem=cs.at[side], recv_sem=cr.at[side],
            device_id={"mode": mode, "space": target}, device_id_type=MESH)

    def halo_copy(it, side):
        target = right_s if side == 0 else left_s
        return pltpu.make_async_remote_copy(
            src_ref=hs_send.at[it, side], dst_ref=hs_recv.at[it, side],
            send_sem=hss.at[it, side], recv_sem=hsr.at[it, side],
            device_id={"mode": mode, "space": target}, device_id_type=MESH)

    def mix(it, ds, first):
        for n, d in enumerate(ds):
            for q in range(NZ):
                hi, lo = split_bf16(ug[it, block(q, d)])
                base = n * 192 + q * IB
                u_st[base:base + IB, :] = hi
                u_st[base + 64:base + 64 + IB, :] = lo
                u_st[base + 128:base + 128 + IB, :] = hi
        for t in range(4):
            cols = slice(t * 256, (t + 1) * 256)
            acc = None
            for n, d in enumerate(ds):
                v = jnp.dot(c_st[SLOT[d % NY]], u_st[n * 192:(n + 1) * 192, cols], preferred_element_type=F32)
                acc = v if acc is None else acc + v
            m_ref[:, cols] = acc if first else m_ref[:, cols] + acc

    def gather(it):
        sent = []

        def msg(number, b, cols, target):
            return pltpu.make_async_remote_copy(
                src_ref=ug.at[it, b, :, cols], dst_ref=ug.at[it, b, :, cols],
                send_sem=gs.at[it, number], recv_sem=gr.at[it, number],
                device_id={"mode": target, "space": space}, device_id_type=MESH)

        def send(number, b, cols, target):
            copy = msg(number, b, cols, target)
            copy.start()
            sent.append(copy)

        def arrive(number, b, cols):
            msg(number, b, cols, yr).wait_recv()

        limit_r, limit_l = [4, 3, 4, 3], [3, 4, 3, 4]

        def a_right(p, q, t):
            send(p * NA + 3 + q * 4 + t - 1, block(q, -(t - 1)), APIECES[p], yr)

        def a_left(p, q, t):
            send(p * NA + 19 + q * 4 + t - 1, block(q, t - 1), APIECES[p], yl)

        def b_z(d):
            for q in ZORDER:
                send(NB0 + 8 + (d % NY) * 3 + q - 1, block(0, d), BPIECE, at_z(q))

        def b_z_arrive(d):
            for q in ZORDER:
                arrive(NB0 + 8 + (d % NY) * 3 + q - 1, block(NZ - q, d), BPIECE)

        def b_r(t):
            send(NB0 + t - 1, block(0, -(t - 1)), BPIECE, yr)

        def b_l(t):
            send(NB0 + 4 + t - 1, block(0, t - 1), BPIECE, yl)

        b_r(1)
        b_l(1)
        for p in range(len(APIECES)):
            a_right(p, 0, 1)
            a_left(p, 0, 1)
            for q in ZORDER:
                send(p * NA + q - 1, mode, APIECES[p], at_z(q))
        b_z(0)
        if it == 0:
            coef_copy(0).start()
            coef_copy(1).start()
        events = [(2.55, 'm', 0, 0, 1), (3.55, 'm', 0, 0, 2), (4.55, 'm', 0, 0, 3)]
        if it == 0:
            events.append((2.6, 'h', 0, 0, 0))
        for p in range(len(APIECES)):
            for q in ZORDER:
                events.append((OFF[NZ - q] + 0.3 * p + 0.01 * ZORDER.index(q), 'z', p, q, 0))
            for q in range(NZ):
                for t in range(1, 5):
                    if t <= limit_r[q]:
                        events.append((OFF[q] + 0.3 * p + t, 'r', p, q, t))
                    if t <= limit_l[q]:
                        events.append((OFF[q] + 0.3 * p + t + 0.001, 'l', p, q, t))
        for t in range(1, 5):
            events.append((t - 0.002, 'br', 0, 0, t))
            if t < 4:
                events.append((t - 0.001, 'bl', 0, 0, t))
        for _, kind, p, q, t in sorted(events):
            if kind == 'z':
                arrive(p * NA + q - 1, block(NZ - q, 0), APIECES[p])
                a_right(p, NZ - q, 1)
                a_left(p, NZ - q, 1)
            elif kind == 'r':
                arrive(p * NA + 3 + q * 4 + t - 1, block(q, -t), APIECES[p])
                if t < limit_r[q]:
                    a_right(p, q, t + 1)
            elif kind == 'l':
                arrive(p * NA + 19 + q * 4 + t - 1, block(q, t), APIECES[p])
                if t < limit_l[q]:
                    a_left(p, q, t + 1)
            elif kind == 'br':
                arrive(NB0 + t - 1, block(0, -t), BPIECE)
                if t < 4:
                    b_r(t + 1)
                b_z(-t)
            elif kind == 'bl':
                arrive(NB0 + 4 + t - 1, block(0, t), BPIECE)
                if t < 3:
                    b_l(t + 1)
                b_z(t)
            elif kind == 'h':
                prepare()
            elif t == 1:
                b_z_arrive(0)
                mix(it, (0,), True)
            else:
                b_z_arrive(t - 1)
                b_z_arrive(1 - t)
                mix(it, (t - 1, 1 - t), False)
        b_z_arrive(3)
        b_z_arrive(-3)
        mix(it, (3, -3), False)
        b_z_arrive(4)
        mix(it, (4,), False)
        return sent

    sub = lax.broadcasted_iota(jnp.int32, (8, 128), 0)
    ysub = lax.rem(sub, 4)
    plane0 = sub < 4

    def prepare():
        coef_copy(0).wait_recv()
        coef_copy(1).wait_recv()
        for k in range(KT):
            al = jnp.where(has_l, a_halo[0, k, 4:8, :], 0.0)
            ar = jnp.where(has_r, a_halo[1, k, 0:4, :], 0.0)
            faces[0, k, 0:4, :] = 0.5 * (a_ref[k, 0:4, :] + al)
            faces[1, k, 4:8, :] = 0.5 * (a_ref[k, 4:8, :] + ar)

        def face_sum(a, x_nb):
            total = x_nb
            total = total + jnp.where(ysub > 0, pltpu.roll(a, 1, 0), 0.0)
            total = total + jnp.where(ysub < 3, pltpu.roll(a, 7, 0), 0.0)
            total = total + lanes_prev(a) + lanes_next(a)
            return 1.0 + 0.5 * (6.0 * a + total)

        a = a_ref[0]
        al = jnp.where(has_l, a_halo[0, 0], 0.0)
        ar = jnp.where(has_r, a_halo[1, 0], 0.0)
        a4, al4, ar4 = pltpu.roll(a, 4, 0), pltpu.roll(al, 4, 0), pltpu.roll(ar, 4, 0)
        dinv[0] = DAMP / face_sum(a, a4 + jnp.where(plane0, al4, ar4))
        dinv[1] = DAMP / face_sum(al, a4 + al4)
        dinv[2] = DAMP / face_sum(ar, a4 + ar4)

    def sums(s):
        acc = None
        for k in range(KT):
            m = m_ref[k * IB:(k + 1) * IB, tile(s)]
            new = [faces[n, k, s:s + 1, :] * m for n in range(6)]
            acc = new if acc is None else [a + b for a, b in zip(acc, new)]
        return acc

    sent = []
    for it in range(ITERS):
        sent += gather(it)
        S = [sums(s) for s in range(8)]
        own = [ug[it, mode, :, tile(s)] for s in range(8)]
        part = []
        for s in range(8):
            xm, xp, ym, yp, zm, zp = S[s]
            ap = (xm + xp) + (ym + yp) + (zm + zp)
            ap = ap - (S[s + 4][0] if s < 4 else S[s - 4][1])
            if s % 4 < 3:
                ap = ap - S[s + 1][2]
            if s % 4 > 0:
                ap = ap - S[s - 1][3]
            ap = ap - lanes_next(zm) - lanes_prev(zp)
            part.append(src_m[:, tile(s)] - own[s] - ap)
        for c in range(4):
            hs_send[it, 0, :, tile(c)] = S[4 + c][1]
            hs_send[it, 0, :, tile(4 + c)] = part[4 + c]
            hs_send[it, 1, :, tile(c)] = S[c][0]
            hs_send[it, 1, :, tile(4 + c)] = part[c]
        halo_copy(it, 0).start()
        halo_copy(it, 1).start()
        halo_copy(it, 0).wait_recv()
        halo_copy(it, 1).wait_recv()
        res, first = [], []
        left_first, right_first = [], []
        for c in range(4):
            res.append(part[c] + jnp.where(has_l, hs_recv[it, 0, :, tile(c)], 0.0))
            v = (hs_recv[it, 0, :, tile(4 + c)] + S[c][0]) * dinv[1, 4 + c:5 + c, :]
            left_first.append(jnp.where(has_l, v, 0.0))
        for c in range(4):
            res.append(part[4 + c] + jnp.where(has_r, hs_recv[it, 1, :, tile(c)], 0.0))
            v = (hs_recv[it, 1, :, tile(4 + c)] + S[4 + c][1]) * dinv[2, c:c + 1, :]
            right_first.append(jnp.where(has_r, v, 0.0))
        for s in range(8):
            first.append(res[s] * dinv[0, s:s + 1, :])
        for s in range(8):
            f = first[s]
            fc = [faces[n, 0, s:s + 1, :] for n in range(6)]
            ap = f
            ap = ap + fc[0] * (f - (first[s - 4] if s >= 4 else left_first[s]))
            ap = ap + fc[1] * (f - (first[s + 4] if s < 4 else right_first[s - 4]))
            ap = ap + fc[2] * (f - first[s - 1] if s % 4 > 0 else f)
            ap = ap + fc[3] * (f - first[s + 1] if s % 4 < 3 else f)
            ap = ap + fc[4] * (f - lanes_prev(f))
            ap = ap + fc[5] * (f - lanes_next(f))
            second = f + (res[s] - ap) * dinv[0, s:s + 1, :]
            new = own[s] + second
            if it + 1 < ITERS:
                ug[it + 1, mode, :, tile(s)] = new
            else:
                po_ref[:, s, :] = new
                ro_ref[:, s, :] = res[s]
    for copy in sent:
        copy.wait_send()
    for side in (0, 1):
        coef_copy(side).wait_send()
        for it in range(ITERS):
            halo_copy(it, side).wait_send()


def on_device(pressure, source, coefficients, coupling):
    vmem, hbm = pl.BlockSpec(memory_space=pltpu.VMEM), pl.BlockSpec(memory_space=pltpu.HBM)
    shape = jax.ShapeDtypeStruct((IB, 8, 128), F32)
    dma = pltpu.SemaphoreType.DMA
    out = pl.pallas_call(
        kernel,
        out_shape=(shape, shape),
        in_specs=[hbm] * 4,
        out_specs=(vmem, vmem),
        scratch_shapes=[
            pltpu.VMEM((IB, 8, 128), F32),
            pltpu.VMEM((IB, 8, 128), F32),
            pltpu.VMEM((KT, 8, 128), F32),
            pltpu.VMEM((PM, PM), F32),
            pltpu.VMEM((ITERS, PM // IB, IB, CELLS), F32),
            pltpu.VMEM((2, KT, 8, 128), F32),
            pltpu.VMEM((NY, PM, 192), BF16),
            pltpu.VMEM((6, KT, 8, 128), F32),
            pltpu.VMEM((3, 8, 128), F32),
            pltpu.VMEM((PM, CELLS), F32),
            pltpu.VMEM((384, CELLS), BF16),
            pltpu.VMEM((ITERS, 2, IB, CELLS), F32),
            pltpu.VMEM((ITERS, 2, IB, CELLS), F32),
            pltpu.VMEM((IB, CELLS), F32),
            dma((4,)),
            dma((ITERS, NMSG)),
            dma((ITERS, NMSG)),
            dma((ITERS, 2)),
            dma((ITERS, 2)),
            dma((2,)),
            dma((2,)),
        ],
        compiler_params=pltpu.CompilerParams(
            collective_id=0, has_side_effects=True, vmem_limit_bytes=66_000_000),
    )(pressure.reshape(IB, 8, 128), source.reshape(IB, 8, 128),
      coefficients.reshape(KT, 8, 128), coupling.reshape(PM, PM))
    return tuple(o.reshape(IB, 2, 4, 128) for o in out)


def solution(mesh):
    return jax.shard_map(
        on_device, mesh=mesh,
        in_specs=(P("mode", "space", None, None), P("mode", "space", None, None),
                  P(None, "space", None, None), P(None, "mode", None)),
        out_specs=(P("mode", "space", None, None), P("mode", "space", None, None)),
        check_vma=False)
```

```python
import functools

import jax
import jax.numpy as jnp
from jax import lax
from jax.experimental import pallas as pl
from jax.experimental.pallas import tpu as pltpu
from jax.sharding import PartitionSpec as P

MESH = pl.DeviceIdType.MESH
ITERS = 2
DAMP = 0.7
KT, IB, PM = 32, 16, 512
NY, NZ = 8, 4
CELLS = 1024
F32, BF16 = jnp.float32, jnp.bfloat16

APIECES = [slice(0, 384), slice(384, 768)]
BPIECE = slice(768, 1024)
ZORDER = (2, 1, 3)
OFF = [0, 0.8, 1.2, 0.8]
NA = 35
NB0 = NA * len(APIECES)
NMSG = NB0 + 32

SLOT = list(range(NY))


def lanes_next(v):
    n = v.shape[-1]
    lane = lax.broadcasted_iota(jnp.int32, v.shape, v.ndim - 1)
    return jnp.where(lane < n - 1, pltpu.roll(v, n - 1, v.ndim - 1), 0.0)


def lanes_prev(v):
    lane = lax.broadcasted_iota(jnp.int32, v.shape, v.ndim - 1)
    return jnp.where(lane > 0, pltpu.roll(v, 1, v.ndim - 1), 0.0)


def split_bf16(x):
    hi = x.astype(BF16)
    return hi, (x - hi.astype(F32)).astype(BF16)


def kernel(u_hbm, src_hbm, a_hbm, c_hbm, po_ref, ro_ref,
           u_ref, src_ref, a_ref, c_ref,
           ug, a_halo, c_st, faces, dinv, m_ref, u_st,
           hs_send, hs_recv, src_m,
           ls, gs, gr, hss, hsr, cs, cr):
    mode, space = lax.axis_index("mode"), lax.axis_index("space")
    ns = lax.axis_size("space")
    zh, y = mode // NY, lax.rem(mode, NY)
    left_s, right_s = lax.rem(space + ns - 1, ns), lax.rem(space + 1, ns)
    yr = zh * NY + lax.rem(y + 1, NY)
    yl = zh * NY + lax.rem(y + NY - 1, NY)
    has_l, has_r = space > 0, space < ns - 1

    def at_z(q):
        return lax.rem(zh + q, NZ) * NY + y

    def block(q, d):
        return lax.rem(zh + q, NZ) * NY + lax.rem(y + NY + d, NY)

    barrier = pltpu.get_barrier_semaphore()
    for target in (yr, yl, at_z(1), at_z(2), at_z(3)):
        pl.semaphore_signal(barrier, inc=1, device_id={"mode": target, "space": space}, device_id_type=MESH)
    for target in (left_s, right_s):
        pl.semaphore_signal(barrier, inc=1, device_id={"mode": mode, "space": target}, device_id_type=MESH)

    loads = [pltpu.make_async_copy(h, v, ls.at[n]) for n, (h, v) in enumerate(
        ((u_hbm, u_ref), (a_hbm, a_ref), (c_hbm, c_ref), (src_hbm, src_ref)))]
    for copy in loads:
        copy.start()

    def tile(s):
        return slice(s * 128, (s + 1) * 128)

    loads[0].wait()
    for s in range(8):
        ug[0, mode, :, tile(s)] = u_ref[:, s, :]
    loads[1].wait()

    def own_faces(k, _):
        a = a_ref[k]
        a4 = pltpu.roll(a, 4, 0)
        sub8 = lax.rem(lax.broadcasted_iota(jnp.int32, (8, 128), 0), 4)
        ym = jnp.where(sub8 > 0, pltpu.roll(a, 1, 0), 0.0)
        yp = jnp.where(sub8 < 3, pltpu.roll(a, 7, 0), 0.0)
        for n, v in enumerate((a4, a4, ym, yp, lanes_prev(a), lanes_next(a))):
            faces[n, k] = 0.5 * (a + v)
        return 0

    lax.fori_loop(0, KT, own_faces, 0, unroll=8)

    loads[2].wait()
    for r in range(8):
        rows = slice(r * 64, (r + 1) * 64)
        hi, lo = [], []
        for q in range(NZ):
            cols = pl.ds(pl.multiple_of(lax.rem(zh + q, NZ) * 128, 128), 128)
            x = pltpu.roll(c_ref[rows, cols], lax.rem(NY - y, NY) * IB, 1)
            h = x.astype(BF16).astype(F32)
            hi.append(h)
            lo.append(x - h)
        for d in range(NY):
            part = slice(d * IB, (d + 1) * IB)
            h = jnp.concatenate([v[:, part] for v in hi], axis=1)
            l = jnp.concatenate([v[:, part] for v in lo], axis=1)
            c_st[SLOT[d], rows, 0:64] = h.astype(BF16)
            c_st[SLOT[d], rows, 64:128] = h.astype(BF16)
            c_st[SLOT[d], rows, 128:192] = l.astype(BF16)
    loads[3].wait()
    for s in range(8):
        src_m[:, tile(s)] = src_ref[:, s, :]
    pl.semaphore_wait(barrier, 7)

    def coef_copy(side):
        target = right_s if side == 0 else left_s
        return pltpu.make_async_remote_copy(
            src_ref=a_ref, dst_ref=a_halo.at[side], send_sem=cs.at[side], recv_sem=cr.at[side],
            device_id={"mode": mode, "space": target}, device_id_type=MESH)

    def halo_copy(it, side):
        target = right_s if side == 0 else left_s
        return pltpu.make_async_remote_copy(
            src_ref=hs_send.at[it, side], dst_ref=hs_recv.at[it, side],
            send_sem=hss.at[it, side], recv_sem=hsr.at[it, side],
            device_id={"mode": mode, "space": target}, device_id_type=MESH)

    def stage(it, ds, cols):
        for n, d in enumerate(ds):
            for q in range(NZ):
                hi, lo = split_bf16(ug[it, block(q, d), :, cols])
                base = n * 192 + q * IB
                u_st[base:base + IB, cols] = hi
                u_st[base + 64:base + 64 + IB, cols] = lo
                u_st[base + 128:base + 128 + IB, cols] = hi

    def product(ds, cols):
        acc = None
        for n, d in enumerate(ds):
            v = jnp.dot(c_st[SLOT[d % NY]], u_st[n * 192:(n + 1) * 192, cols], preferred_element_type=F32)
            acc = v if acc is None else acc + v
        return acc

    def mix(it, ds, first):
        stage(it, ds, slice(0, CELLS))
        for t in range(4):
            cols = slice(t * 256, (t + 1) * 256)
            acc = product(ds, cols)
            m_ref[:, cols] = acc if first else m_ref[:, cols] + acc

    def last(it, cols):
        stage(it, (4,), cols)
        m_ref[:, cols] = m_ref[:, cols] + product((4,), cols)
        return [sums(s) for s in range(cols.start // 128, cols.stop // 128)]

    def gather(it):
        sent = []

        def msg(number, b, cols, target):
            return pltpu.make_async_remote_copy(
                src_ref=ug.at[it, b, :, cols], dst_ref=ug.at[it, b, :, cols],
                send_sem=gs.at[it, number], recv_sem=gr.at[it, number],
                device_id={"mode": target, "space": space}, device_id_type=MESH)

        def send(number, b, cols, target):
            copy = msg(number, b, cols, target)
            copy.start()
            sent.append(copy)

        def arrive(number, b, cols):
            msg(number, b, cols, yr).wait_recv()

        limit_r, limit_l = [4, 3, 4, 3], [3, 4, 3, 4]

        def a_right(p, q, t):
            send(p * NA + 3 + q * 4 + t - 1, block(q, -(t - 1)), APIECES[p], yr)

        def a_left(p, q, t):
            send(p * NA + 19 + q * 4 + t - 1, block(q, t - 1), APIECES[p], yl)

        def b_z(d):
            for q in ZORDER:
                send(NB0 + 8 + (d % NY) * 3 + q - 1, block(0, d), BPIECE, at_z(q))

        def b_z_arrive(d):
            for q in ZORDER:
                arrive(NB0 + 8 + (d % NY) * 3 + q - 1, block(NZ - q, d), BPIECE)

        def b_r(t):
            send(NB0 + t - 1, block(0, -(t - 1)), BPIECE, yr)

        def b_l(t):
            send(NB0 + 4 + t - 1, block(0, t - 1), BPIECE, yl)

        b_r(1)
        b_l(1)
        for p in range(len(APIECES)):
            a_right(p, 0, 1)
            a_left(p, 0, 1)
            for q in ZORDER:
                send(p * NA + q - 1, mode, APIECES[p], at_z(q))
        b_z(0)
        if it == 0:
            coef_copy(0).start()
            coef_copy(1).start()
        events = [(2.55, 'm', 0, 0, 1), (3.55, 'm', 0, 0, 2), (4.55, 'm', 0, 0, 3), (4.79, 'm', 0, 0, 4)]
        face_sums = []
        if it == 0:
            events.append((2.6, 'h', 0, 0, 0))
        for p in range(len(APIECES)):
            for q in ZORDER:
                events.append((OFF[NZ - q] + 0.3 * p + 0.01 * ZORDER.index(q), 'z', p, q, 0))
            for q in range(NZ):
                for t in range(1, 5):
                    w = OFF[q] + 0.3 * p + t if t < 4 else 5 + p + 0.1 * OFF[q]
                    if t <= limit_r[q]:
                        events.append((w, 'r', p, q, t))
                    if t <= limit_l[q]:
                        events.append((w + 0.001, 'l', p, q, t))
            events.append((5.5 + p, 's', p, 0, 0))
        for t in range(1, 5):
            events.append((t - 0.002, 'br', 0, 0, t))
            if t < 4:
                events.append((t - 0.001, 'bl', 0, 0, t))
        for _, kind, p, q, t in sorted(events):
            if kind == 'z':
                arrive(p * NA + q - 1, block(NZ - q, 0), APIECES[p])
                a_right(p, NZ - q, 1)
                a_left(p, NZ - q, 1)
            elif kind == 'r':
                arrive(p * NA + 3 + q * 4 + t - 1, block(q, -t), APIECES[p])
                if t < limit_r[q]:
                    a_right(p, q, t + 1)
            elif kind == 'l':
                arrive(p * NA + 19 + q * 4 + t - 1, block(q, t), APIECES[p])
                if t < limit_l[q]:
                    a_left(p, q, t + 1)
            elif kind == 'br':
                arrive(NB0 + t - 1, block(0, -t), BPIECE)
                if t < 4:
                    b_r(t + 1)
                b_z(-t)
            elif kind == 'bl':
                arrive(NB0 + 4 + t - 1, block(0, t), BPIECE)
                if t < 3:
                    b_l(t + 1)
                b_z(t)
            elif kind == 'h':
                prepare()
            elif kind == 's':
                face_sums += last(it, APIECES[p])
            elif t == 1:
                b_z_arrive(0)
                mix(it, (0,), True)
            else:
                b_z_arrive(t - 1)
                b_z_arrive(1 - t)
                mix(it, (t - 1, 1 - t), False)
        b_z_arrive(4)
        face_sums += last(it, BPIECE)
        return sent, face_sums

    sub = lax.broadcasted_iota(jnp.int32, (8, 128), 0)
    ysub = lax.rem(sub, 4)
    plane0 = sub < 4

    def prepare():
        coef_copy(0).wait_recv()
        coef_copy(1).wait_recv()
        for k in range(KT):
            al = jnp.where(has_l, a_halo[0, k, 4:8, :], 0.0)
            ar = jnp.where(has_r, a_halo[1, k, 0:4, :], 0.0)
            faces[0, k, 0:4, :] = 0.5 * (a_ref[k, 0:4, :] + al)
            faces[1, k, 4:8, :] = 0.5 * (a_ref[k, 4:8, :] + ar)

        def face_sum(a, x_nb):
            total = x_nb
            total = total + jnp.where(ysub > 0, pltpu.roll(a, 1, 0), 0.0)
            total = total + jnp.where(ysub < 3, pltpu.roll(a, 7, 0), 0.0)
            total = total + lanes_prev(a) + lanes_next(a)
            return 1.0 + 0.5 * (6.0 * a + total)

        a = a_ref[0]
        al = jnp.where(has_l, a_halo[0, 0], 0.0)
        ar = jnp.where(has_r, a_halo[1, 0], 0.0)
        a4, al4, ar4 = pltpu.roll(a, 4, 0), pltpu.roll(al, 4, 0), pltpu.roll(ar, 4, 0)
        dinv[0] = DAMP / face_sum(a, a4 + jnp.where(plane0, al4, ar4))
        dinv[1] = DAMP / face_sum(al, a4 + al4)
        dinv[2] = DAMP / face_sum(ar, a4 + ar4)

    def sums(s):
        acc = None
        for k in range(KT):
            m = m_ref[k * IB:(k + 1) * IB, tile(s)]
            new = [faces[n, k, s:s + 1, :] * m for n in range(6)]
            acc = new if acc is None else [a + b for a, b in zip(acc, new)]
        return acc

    sent = []
    for it in range(ITERS):
        copies, S = gather(it)
        sent += copies
        own = [ug[it, mode, :, tile(s)] for s in range(8)]
        part = []
        for s in range(8):
            xm, xp, ym, yp, zm, zp = S[s]
            ap = (xm + xp) + (ym + yp) + (zm + zp)
            ap = ap - (S[s + 4][0] if s < 4 else S[s - 4][1])
            if s % 4 < 3:
                ap = ap - S[s + 1][2]
            if s % 4 > 0:
                ap = ap - S[s - 1][3]
            ap = ap - lanes_next(zm) - lanes_prev(zp)
            part.append(src_m[:, tile(s)] - own[s] - ap)
        for c in range(4):
            hs_send[it, 0, :, tile(c)] = S[4 + c][1]
            hs_send[it, 0, :, tile(4 + c)] = part[4 + c]
            hs_send[it, 1, :, tile(c)] = S[c][0]
            hs_send[it, 1, :, tile(4 + c)] = part[c]
        halo_copy(it, 0).start()
        halo_copy(it, 1).start()
        halo_copy(it, 0).wait_recv()
        halo_copy(it, 1).wait_recv()
        res, first = [], []
        left_first, right_first = [], []
        for c in range(4):
            res.append(part[c] + jnp.where(has_l, hs_recv[it, 0, :, tile(c)], 0.0))
            v = (hs_recv[it, 0, :, tile(4 + c)] + S[c][0]) * dinv[1, 4 + c:5 + c, :]
            left_first.append(jnp.where(has_l, v, 0.0))
        for c in range(4):
            res.append(part[4 + c] + jnp.where(has_r, hs_recv[it, 1, :, tile(c)], 0.0))
            v = (hs_recv[it, 1, :, tile(4 + c)] + S[4 + c][1]) * dinv[2, c:c + 1, :]
            right_first.append(jnp.where(has_r, v, 0.0))
        for s in range(8):
            first.append(res[s] * dinv[0, s:s + 1, :])
        for s in range(8):
            f = first[s]
            fc = [faces[n, 0, s:s + 1, :] for n in range(6)]
            ap = f
            ap = ap + fc[0] * (f - (first[s - 4] if s >= 4 else left_first[s]))
            ap = ap + fc[1] * (f - (first[s + 4] if s < 4 else right_first[s - 4]))
            ap = ap + fc[2] * (f - first[s - 1] if s % 4 > 0 else f)
            ap = ap + fc[3] * (f - first[s + 1] if s % 4 < 3 else f)
            ap = ap + fc[4] * (f - lanes_prev(f))
            ap = ap + fc[5] * (f - lanes_next(f))
            second = f + (res[s] - ap) * dinv[0, s:s + 1, :]
            new = own[s] + second
            if it + 1 < ITERS:
                ug[it + 1, mode, :, tile(s)] = new
            else:
                po_ref[:, s, :] = new
                ro_ref[:, s, :] = res[s]
    for copy in sent:
        copy.wait_send()
    for side in (0, 1):
        coef_copy(side).wait_send()
        for it in range(ITERS):
            halo_copy(it, side).wait_send()


def on_device(pressure, source, coefficients, coupling):
    vmem, hbm = pl.BlockSpec(memory_space=pltpu.VMEM), pl.BlockSpec(memory_space=pltpu.HBM)
    shape = jax.ShapeDtypeStruct((IB, 8, 128), F32)
    dma = pltpu.SemaphoreType.DMA
    out = pl.pallas_call(
        kernel,
        out_shape=(shape, shape),
        in_specs=[hbm] * 4,
        out_specs=(vmem, vmem),
        scratch_shapes=[
            pltpu.VMEM((IB, 8, 128), F32),
            pltpu.VMEM((IB, 8, 128), F32),
            pltpu.VMEM((KT, 8, 128), F32),
            pltpu.VMEM((PM, PM), F32),
            pltpu.VMEM((ITERS, PM // IB, IB, CELLS), F32),
            pltpu.VMEM((2, KT, 8, 128), F32),
            pltpu.VMEM((NY, PM, 192), BF16),
            pltpu.VMEM((6, KT, 8, 128), F32),
            pltpu.VMEM((3, 8, 128), F32),
            pltpu.VMEM((PM, CELLS), F32),
            pltpu.VMEM((384, CELLS), BF16),
            pltpu.VMEM((ITERS, 2, IB, CELLS), F32),
            pltpu.VMEM((ITERS, 2, IB, CELLS), F32),
            pltpu.VMEM((IB, CELLS), F32),
            dma((4,)),
            dma((ITERS, NMSG)),
            dma((ITERS, NMSG)),
            dma((ITERS, 2)),
            dma((ITERS, 2)),
            dma((2,)),
            dma((2,)),
        ],
        compiler_params=pltpu.CompilerParams(
            collective_id=0, has_side_effects=True, vmem_limit_bytes=66_000_000),
    )(pressure.reshape(IB, 8, 128), source.reshape(IB, 8, 128),
      coefficients.reshape(KT, 8, 128), coupling.reshape(PM, PM))
    return tuple(o.reshape(IB, 2, 4, 128) for o in out)


def solution(mesh):
    return jax.shard_map(
        on_device, mesh=mesh,
        in_specs=(P("mode", "space", None, None), P("mode", "space", None, None),
                  P(None, "space", None, None), P(None, "mode", None)),
        out_specs=(P("mode", "space", None, None), P("mode", "space", None, None)),
        check_vma=False)
```

```python
import functools

import jax
import jax.numpy as jnp
from jax import lax
from jax.experimental import pallas as pl
from jax.experimental.pallas import tpu as pltpu
from jax.sharding import PartitionSpec as P

MESH = pl.DeviceIdType.MESH
ITERS = 2
DAMP = 0.7
KT, IB, PM = 32, 16, 512
NY, NZ = 8, 4
CELLS = 1024
F32, BF16 = jnp.float32, jnp.bfloat16

APIECES = [slice(0, 384), slice(384, 768)]
BPIECE = slice(768, 1024)
ZORDER = (2, 1, 3)
OFF = [0, 0.8, 1.2, 0.8]
NA = 35
NB0 = NA * len(APIECES)
NMSG = NB0 + 32

SLOT = list(range(NY))


def lanes_next(v):
    n = v.shape[-1]
    lane = lax.broadcasted_iota(jnp.int32, v.shape, v.ndim - 1)
    return jnp.where(lane < n - 1, pltpu.roll(v, n - 1, v.ndim - 1), 0.0)


def lanes_prev(v):
    lane = lax.broadcasted_iota(jnp.int32, v.shape, v.ndim - 1)
    return jnp.where(lane > 0, pltpu.roll(v, 1, v.ndim - 1), 0.0)


def split_bf16(x):
    hi = x.astype(BF16)
    return hi, (x - hi.astype(F32)).astype(BF16)


def kernel(u_hbm, src_hbm, a_hbm, c_hbm, po_ref, ro_ref,
           u_ref, src_ref, a_ref, c_ref,
           ug, a_halo, c_st, faces, dinv, m_ref, u_st,
           hs_send, hs_recv, src_m,
           ls, gs, gr, hss, hsr, cs, cr):
    mode, space = lax.axis_index("mode"), lax.axis_index("space")
    ns = lax.axis_size("space")
    zh, y = mode // NY, lax.rem(mode, NY)
    left_s, right_s = lax.rem(space + ns - 1, ns), lax.rem(space + 1, ns)
    yr = zh * NY + lax.rem(y + 1, NY)
    yl = zh * NY + lax.rem(y + NY - 1, NY)
    has_l, has_r = space > 0, space < ns - 1

    def at_z(q):
        return lax.rem(zh + q, NZ) * NY + y

    def block(q, d):
        return lax.rem(zh + q, NZ) * NY + lax.rem(y + NY + d, NY)

    barrier = pltpu.get_barrier_semaphore()
    for target in (yr, yl, at_z(1), at_z(2), at_z(3)):
        pl.semaphore_signal(barrier, inc=1, device_id={"mode": target, "space": space}, device_id_type=MESH)
    for target in (left_s, right_s):
        pl.semaphore_signal(barrier, inc=1, device_id={"mode": mode, "space": target}, device_id_type=MESH)

    loads = [pltpu.make_async_copy(h, v, ls.at[n]) for n, (h, v) in enumerate(
        ((u_hbm, u_ref), (a_hbm, a_ref), (c_hbm, c_ref), (src_hbm, src_ref)))]
    for copy in loads:
        copy.start()

    def tile(s):
        return slice(s * 128, (s + 1) * 128)

    loads[0].wait()
    for s in range(8):
        ug[0, mode, :, tile(s)] = u_ref[:, s, :]
    loads[1].wait()

    def own_faces(k, _):
        a = a_ref[k]
        a4 = pltpu.roll(a, 4, 0)
        sub8 = lax.rem(lax.broadcasted_iota(jnp.int32, (8, 128), 0), 4)
        ym = jnp.where(sub8 > 0, pltpu.roll(a, 1, 0), 0.0)
        yp = jnp.where(sub8 < 3, pltpu.roll(a, 7, 0), 0.0)
        for n, v in enumerate((a4, a4, ym, yp, lanes_prev(a), lanes_next(a))):
            faces[n, k] = 0.5 * (a + v)
        return 0

    lax.fori_loop(0, KT, own_faces, 0, unroll=8)

    loads[2].wait()
    for r in range(8):
        rows = slice(r * 64, (r + 1) * 64)
        hi, lo = [], []
        for q in range(NZ):
            cols = pl.ds(pl.multiple_of(lax.rem(zh + q, NZ) * 128, 128), 128)
            x = pltpu.roll(c_ref[rows, cols], lax.rem(NY - y, NY) * IB, 1)
            h = x.astype(BF16).astype(F32)
            hi.append(h)
            lo.append(x - h)
        for d in range(NY):
            part = slice(d * IB, (d + 1) * IB)
            h = jnp.concatenate([v[:, part] for v in hi], axis=1)
            l = jnp.concatenate([v[:, part] for v in lo], axis=1)
            c_st[SLOT[d], rows, 0:64] = h.astype(BF16)
            c_st[SLOT[d], rows, 64:128] = h.astype(BF16)
            c_st[SLOT[d], rows, 128:192] = l.astype(BF16)
    loads[3].wait()
    for s in range(8):
        src_m[:, tile(s)] = src_ref[:, s, :]
    pl.semaphore_wait(barrier, 7)

    def coef_copy(side):
        target = right_s if side == 0 else left_s
        return pltpu.make_async_remote_copy(
            src_ref=a_ref, dst_ref=a_halo.at[side], send_sem=cs.at[side], recv_sem=cr.at[side],
            device_id={"mode": mode, "space": target}, device_id_type=MESH)

    def halo_copy(it, side):
        target = right_s if side == 0 else left_s
        return pltpu.make_async_remote_copy(
            src_ref=hs_send.at[it, side], dst_ref=hs_recv.at[it, side],
            send_sem=hss.at[it, side], recv_sem=hsr.at[it, side],
            device_id={"mode": mode, "space": target}, device_id_type=MESH)

    def stage(it, ds, cols):
        for n, d in enumerate(ds):
            for q in range(NZ):
                hi, lo = split_bf16(ug[it, block(q, d), :, cols])
                base = n * 192 + q * IB
                u_st[base:base + IB, cols] = hi
                u_st[base + 64:base + 64 + IB, cols] = lo
                u_st[base + 128:base + 128 + IB, cols] = hi

    def product(ds, cols):
        acc = None
        for n, d in enumerate(ds):
            v = jnp.dot(c_st[SLOT[d % NY]], u_st[n * 192:(n + 1) * 192, cols], preferred_element_type=F32)
            acc = v if acc is None else acc + v
        return acc

    def mix(it, ds, first):
        stage(it, ds, slice(0, CELLS))
        for t in range(4):
            cols = slice(t * 256, (t + 1) * 256)
            acc = product(ds, cols)
            m_ref[:, cols] = acc if first else m_ref[:, cols] + acc

    def last(it, cols):
        stage(it, (4,), cols)
        m_ref[:, cols] = m_ref[:, cols] + product((4,), cols)
        return [sums(s) for s in range(cols.start // 128, cols.stop // 128)]

    def gather(it):
        sent = []

        def msg(number, b, cols, target):
            return pltpu.make_async_remote_copy(
                src_ref=ug.at[it, b, :, cols], dst_ref=ug.at[it, b, :, cols],
                send_sem=gs.at[it, number], recv_sem=gr.at[it, number],
                device_id={"mode": target, "space": space}, device_id_type=MESH)

        def send(number, b, cols, target):
            copy = msg(number, b, cols, target)
            copy.start()
            sent.append(copy)

        def arrive(number, b, cols):
            msg(number, b, cols, yr).wait_recv()

        limit_r, limit_l = [4, 3, 4, 3], [3, 4, 3, 4]

        def a_right(p, q, t):
            send(p * NA + 3 + q * 4 + t - 1, block(q, -(t - 1)), APIECES[p], yr)

        def a_left(p, q, t):
            send(p * NA + 19 + q * 4 + t - 1, block(q, t - 1), APIECES[p], yl)

        def b_z(d):
            for q in ZORDER:
                send(NB0 + 8 + (d % NY) * 3 + q - 1, block(0, d), BPIECE, at_z(q))

        def b_z_arrive(d):
            for q in ZORDER:
                arrive(NB0 + 8 + (d % NY) * 3 + q - 1, block(NZ - q, d), BPIECE)

        def b_r(t):
            send(NB0 + t - 1, block(0, -(t - 1)), BPIECE, yr)

        def b_l(t):
            send(NB0 + 4 + t - 1, block(0, t - 1), BPIECE, yl)

        b_r(1)
        b_l(1)
        for p in range(len(APIECES)):
            a_right(p, 0, 1)
            a_left(p, 0, 1)
            for q in ZORDER:
                send(p * NA + q - 1, mode, APIECES[p], at_z(q))
        b_z(0)
        if it == 0:
            coef_copy(0).start()
            coef_copy(1).start()
        events = [(2.55, 'm', 0, 0, 1), (3.55, 'm', 0, 0, 2), (4.55, 'm', 0, 0, 3), (4.79, 'm', 0, 0, 4)]
        face_sums = []
        if it == 0:
            events.append((2.6, 'h', 0, 0, 0))
        for p in range(len(APIECES)):
            for q in ZORDER:
                events.append((OFF[NZ - q] + 0.3 * p + 0.01 * ZORDER.index(q), 'z', p, q, 0))
            for q in range(NZ):
                for t in range(1, 5):
                    w = OFF[q] + 0.3 * p + t if t < 4 else 5 + p + 0.1 * OFF[q]
                    if t <= limit_r[q]:
                        events.append((w, 'r', p, q, t))
                    if t <= limit_l[q]:
                        events.append((w + 0.001, 'l', p, q, t))
            events.append((5.5 + p, 's', p, 0, 0))
        for t in range(1, 5):
            events.append((t - 0.002, 'br', 0, 0, t))
            if t < 4:
                events.append((t - 0.001, 'bl', 0, 0, t))
        for _, kind, p, q, t in sorted(events):
            if kind == 'z':
                arrive(p * NA + q - 1, block(NZ - q, 0), APIECES[p])
                a_right(p, NZ - q, 1)
                a_left(p, NZ - q, 1)
            elif kind == 'r':
                arrive(p * NA + 3 + q * 4 + t - 1, block(q, -t), APIECES[p])
                if t < limit_r[q]:
                    a_right(p, q, t + 1)
            elif kind == 'l':
                arrive(p * NA + 19 + q * 4 + t - 1, block(q, t), APIECES[p])
                if t < limit_l[q]:
                    a_left(p, q, t + 1)
            elif kind == 'br':
                arrive(NB0 + t - 1, block(0, -t), BPIECE)
                if t < 4:
                    b_r(t + 1)
                b_z(-t)
            elif kind == 'bl':
                arrive(NB0 + 4 + t - 1, block(0, t), BPIECE)
                if t < 3:
                    b_l(t + 1)
                b_z(t)
            elif kind == 'h':
                prepare()
            elif kind == 's':
                face_sums += last(it, APIECES[p])
            elif t == 1:
                b_z_arrive(0)
                mix(it, (0,), True)
            else:
                b_z_arrive(t - 1)
                b_z_arrive(1 - t)
                mix(it, (t - 1, 1 - t), False)
        b_z_arrive(4)
        face_sums += last(it, BPIECE)
        return sent, face_sums

    sub = lax.broadcasted_iota(jnp.int32, (8, 128), 0)
    ysub = lax.rem(sub, 4)
    plane0 = sub < 4

    def prepare():
        coef_copy(0).wait_recv()
        coef_copy(1).wait_recv()
        for k in range(KT):
            al = jnp.where(has_l, a_halo[0, k, 4:8, :], 0.0)
            ar = jnp.where(has_r, a_halo[1, k, 0:4, :], 0.0)
            faces[0, k, 0:4, :] = 0.5 * (a_ref[k, 0:4, :] + al)
            faces[1, k, 4:8, :] = 0.5 * (a_ref[k, 4:8, :] + ar)

        def face_sum(a, x_nb):
            total = x_nb
            total = total + jnp.where(ysub > 0, pltpu.roll(a, 1, 0), 0.0)
            total = total + jnp.where(ysub < 3, pltpu.roll(a, 7, 0), 0.0)
            total = total + lanes_prev(a) + lanes_next(a)
            return 1.0 + 0.5 * (6.0 * a + total)

        a = a_ref[0]
        al = jnp.where(has_l, a_halo[0, 0], 0.0)
        ar = jnp.where(has_r, a_halo[1, 0], 0.0)
        a4, al4, ar4 = pltpu.roll(a, 4, 0), pltpu.roll(al, 4, 0), pltpu.roll(ar, 4, 0)
        dinv[0] = DAMP / face_sum(a, a4 + jnp.where(plane0, al4, ar4))
        dinv[1] = DAMP / face_sum(al, a4 + al4)
        dinv[2] = DAMP / face_sum(ar, a4 + ar4)

    def sums(s):
        acc = None
        for k in range(KT):
            m = m_ref[k * IB:(k + 1) * IB, tile(s)]
            new = [faces[n, k, s:s + 1, :] * m for n in range(6)]
            acc = new if acc is None else [a + b for a, b in zip(acc, new)]
        return acc

    sent = []
    for it in range(ITERS):
        copies, S = gather(it)
        sent += copies
        own = [ug[it, mode, :, tile(s)] for s in range(8)]
        part = []
        for s in range(8):
            xm, xp, ym, yp, zm, zp = S[s]
            ap = (xm + xp) + (ym + yp) + (zm + zp)
            ap = ap - (S[s + 4][0] if s < 4 else S[s - 4][1])
            if s % 4 < 3:
                ap = ap - S[s + 1][2]
            if s % 4 > 0:
                ap = ap - S[s - 1][3]
            ap = ap - lanes_next(zm) - lanes_prev(zp)
            part.append(src_m[:, tile(s)] - own[s] - ap)
        for c in range(4):
            hs_send[it, 0, :, tile(c)] = S[4 + c][1]
            hs_send[it, 0, :, tile(4 + c)] = part[4 + c]
            hs_send[it, 1, :, tile(c)] = S[c][0]
            hs_send[it, 1, :, tile(4 + c)] = part[c]
        halo_copy(it, 0).start()
        halo_copy(it, 1).start()
        halo_copy(it, 0).wait_recv()
        halo_copy(it, 1).wait_recv()
        res, first = [], []
        left_first, right_first = [], []
        for c in range(4):
            res.append(part[c] + jnp.where(has_l, hs_recv[it, 0, :, tile(c)], 0.0))
            v = (hs_recv[it, 0, :, tile(4 + c)] + S[c][0]) * dinv[1, 4 + c:5 + c, :]
            left_first.append(jnp.where(has_l, v, 0.0))
        for c in range(4):
            res.append(part[4 + c] + jnp.where(has_r, hs_recv[it, 1, :, tile(c)], 0.0))
            v = (hs_recv[it, 1, :, tile(4 + c)] + S[4 + c][1]) * dinv[2, c:c + 1, :]
            right_first.append(jnp.where(has_r, v, 0.0))
        for s in range(8):
            first.append(res[s] * dinv[0, s:s + 1, :])
        for s in range(8):
            f = first[s]
            fc = [faces[n, 0, s:s + 1, :] for n in range(6)]
            ap = f
            ap = ap + fc[0] * (f - (first[s - 4] if s >= 4 else left_first[s]))
            ap = ap + fc[1] * (f - (first[s + 4] if s < 4 else right_first[s - 4]))
            ap = ap + fc[2] * (f - first[s - 1] if s % 4 > 0 else f)
            ap = ap + fc[3] * (f - first[s + 1] if s % 4 < 3 else f)
            ap = ap + fc[4] * (f - lanes_prev(f))
            ap = ap + fc[5] * (f - lanes_next(f))
            second = f + (res[s] - ap) * dinv[0, s:s + 1, :]
            new = own[s] + second
            if it + 1 < ITERS:
                ug[it + 1, mode, :, tile(s)] = new
            else:
                po_ref[:, s, :] = new
                ro_ref[:, s, :] = res[s]
    for copy in sent:
        copy.wait_send()
    for side in (0, 1):
        coef_copy(side).wait_send()
        for it in range(ITERS):
            halo_copy(it, side).wait_send()


def hand_on(a_ref, b_ref, c_ref, d_ref):
    c_ref[...] = a_ref[...]
    d_ref[...] = b_ref[...]


def on_device(pressure, source, coefficients, coupling):
    vmem, hbm = pl.BlockSpec(memory_space=pltpu.VMEM), pl.BlockSpec(memory_space=pltpu.HBM)
    shape = jax.ShapeDtypeStruct((IB, 8, 128), F32)
    dma = pltpu.SemaphoreType.DMA
    out = pl.pallas_call(
        kernel,
        out_shape=(shape, shape),
        in_specs=[hbm] * 4,
        out_specs=(vmem, vmem),
        scratch_shapes=[
            pltpu.VMEM((IB, 8, 128), F32),
            pltpu.VMEM((IB, 8, 128), F32),
            pltpu.VMEM((KT, 8, 128), F32),
            pltpu.VMEM((PM, PM), F32),
            pltpu.VMEM((ITERS, PM // IB, IB, CELLS), F32),
            pltpu.VMEM((2, KT, 8, 128), F32),
            pltpu.VMEM((NY, PM, 192), BF16),
            pltpu.VMEM((6, KT, 8, 128), F32),
            pltpu.VMEM((3, 8, 128), F32),
            pltpu.VMEM((PM, CELLS), F32),
            pltpu.VMEM((384, CELLS), BF16),
            pltpu.VMEM((ITERS, 2, IB, CELLS), F32),
            pltpu.VMEM((ITERS, 2, IB, CELLS), F32),
            pltpu.VMEM((IB, CELLS), F32),
            dma((4,)),
            dma((ITERS, NMSG)),
            dma((ITERS, NMSG)),
            dma((ITERS, 2)),
            dma((ITERS, 2)),
            dma((2,)),
            dma((2,)),
        ],
        compiler_params=pltpu.CompilerParams(
            collective_id=0, has_side_effects=True, vmem_limit_bytes=66_000_000),
    )(pressure.reshape(IB, 8, 128), source.reshape(IB, 8, 128),
      coefficients.reshape(KT, 8, 128), coupling.reshape(PM, PM))
    out = pl.pallas_call(
        hand_on, out_shape=(shape, shape), in_specs=[vmem] * 2, out_specs=(vmem, vmem))(*out)
    return tuple(o.reshape(IB, 2, 4, 128) for o in out)


def solution(mesh):
    return jax.shard_map(
        on_device, mesh=mesh,
        in_specs=(P("mode", "space", None, None), P("mode", "space", None, None),
                  P(None, "space", None, None), P(None, "mode", None)),
        out_specs=(P("mode", "space", None, None), P("mode", "space", None, None)),
        check_vma=False)
```
